32 devices in a mesh: island: 16 (over z, y, x), tensor: 2 (over core).
Axes of the slice: x: 2, y: 2, z: 4, core: 2. Of those that a mesh axis runs over, the one named last changes fastest.
Arguments:
- pseudo_grad: float32 [16, 32, 53248], P('island', None, 'tensor'), may hold values from -8000 to 8000
- outer_params: float32 [32, 53248], P('island', 'tensor'), may hold values from -4 to 4
- momentum: float32 [32, 53248], P('island', 'tensor'), may hold values from -6 to 6
- save_pages: int32 [16], replicated, may hold values from 1 to 832, 6656 in all
- writer: int32 [16], replicated, may hold values from 0 to 15, each once
Outputs:
- new_master: float32 [32, 53248], P('island', 'tensor')
- new_momentum: float32 [32, 53248], P('island', 'tensor')
- checkpoint: bfloat16 [16, 832, 256], P('island', None, 'tensor')
The draws below stay inside these ranges and needn't reach their ends.
Inputs may be any that keep to these rules, and one draw needn't show every extreme that they name: save_pages sums to 6656; the longest range has exactly 832 pages. writer names every island once.
All inputs are finite; a program needn't handle non-finite values.
Results may differ from the reference program's by a relative error of at most 0.0007.
Values may be sent and summed in bfloat16 or wider, within the bound.
A program may use at most 64 MiB of HBM per device.

```python
import math
import jax
import jax.numpy as jnp
import numpy as np
from jax import lax

FF = 53248
ISLANDS = 16
ROWS = 32
PAGES = 6656
CAP = 832
N_TENSOR = 2


def draw_pseudo_grad(key, part):
    keys = jax.random.split(jax.random.fold_in(key, 17), 3)
    base = jax.random.truncated_normal(keys[0], -6.0, 6.0, (ISLANDS, ROWS, FF), jnp.float32)
    row_scale = jnp.exp(jax.random.uniform(keys[1], (ROWS,), jnp.float32, 0.0, math.log(10.0)))
    row_scale = row_scale * jnp.exp(math.log(3.0) * jnp.arange(ROWS, dtype=jnp.float32) / ROWS)
    col_scale = jnp.exp(jax.random.uniform(keys[2], (FF,), jnp.float32, 0.0, math.log(10.0)))
    col_scale = col_scale * jnp.exp(math.log(3.0) * jnp.arange(FF, dtype=jnp.float32) / FF)
    return base * row_scale[None, :, None] * col_scale[None, None, :]


def block_scale(key, dims, cuts, low, top_value):
    gain, own = 1.0, jax.random.fold_in(key, 6)
    for dim, blocks in cuts:
        steps = jnp.exp(jax.random.uniform(jax.random.fold_in(own, dim), (blocks,), jnp.float32, low / len(cuts), top_value / len(cuts)))
        gain = gain * jnp.repeat(steps, dims[dim] // blocks).reshape([-1 if axis == dim else 1 for axis in range(len(dims))])
    return gain


def profile(amount, total, most, lean):
    portions = [(1 << 20) // math.isqrt(grade ** lean) + 1 for grade in range(2, amount + 1)]
    surplus, given = total - most - (amount - 1), [1] * (amount - 1)
    while surplus > 0:
        candidates = [i for i in range(amount - 1) if given[i] < most]
        whole, remaining = sum([portions[i] for i in candidates]), surplus
        for i in candidates:
            more = min(most - given[i], max(1, remaining * portions[i] // whole), surplus)
            given[i] = given[i] + more
            surplus = surplus - more
    return np.array([most] + given)


def ragged(rng, amount, total, reach, slope):
    if amount == 2:
        one = jax.random.randint(rng, (), max(1, total - reach), min(reach, total - 1) + 1)
        return jnp.stack([one, total - one])
    tallies = jnp.asarray(profile(amount, total, reach, slope), jnp.int32)
    couples = (amount - 1) // 2
    source_of, receiver = tallies[1:1 + 2 * couples:2], tallies[2:2 + 2 * couples:2]
    margin = jnp.minimum(source_of - 1, reach - receiver)
    passed = jax.random.randint(jax.random.fold_in(rng, 1), (couples,), 0, 1 << 20) % (margin + 1)
    tallies = tallies.at[1:1 + 2 * couples:2].set(source_of - passed).at[2:2 + 2 * couples:2].set(receiver + passed)
    return tallies[jax.random.permutation(jax.random.fold_in(rng, 2), amount)]


def noise(stream_key, dims, width, bound, cuts=(), kind=jnp.bfloat16):
    array = jax.random.normal(stream_key, dims, jnp.float32) * width
    if len(cuts) > 0:
        array = block_scale(stream_key, dims, cuts, -0.22, 0.18) * array
    return jnp.clip(array, min=-bound, max=bound).astype(kind)


def setup_inputs(seed: int = 0) -> dict:
    key_of = jax.random.split(jax.random.key(seed), 6)
    return {
        "pseudo_grad": draw_pseudo_grad(jax.random.fold_in(key_of[5], 71), 0),
        "outer_params": noise(key_of[1], (ROWS, FF), 0.5, 4.0, ((0, 16), (1, 2)), jnp.float32),
        "momentum": noise(key_of[2], (ROWS, FF), 1.0, 6.0, ((0, 16), (1, 2)), jnp.float32),
        "save_pages": ragged(key_of[3], ISLANDS, PAGES, CAP, 2).astype(jnp.int32),
        "writer": jax.random.permutation(key_of[4], ISLANDS).astype(jnp.int32),
    }


epsilon = 1e-06
decay_rate = 0.9
outer_rate = 0.7

def reference(pseudo_grad, outer_params, momentum, save_pages, writer):

    def add_island(island_id, running):
        return running + pseudo_grad[island_id]
    summed = lax.fori_loop(0, ISLANDS, add_island, jnp.zeros((ROWS, FF), jnp.float32))
    outer_grad = summed / ISLANDS
    square_sum = jnp.sum(outer_grad * outer_grad)
    normed = outer_grad / jnp.sqrt(square_sum / (ROWS * FF) + epsilon)
    new_momentum = decay_rate * momentum + normed
    new_master = outer_params - outer_rate * (normed + decay_rate * new_momentum)
    cast_rows = new_master.astype(jnp.bfloat16)
    shards = FF // N_TENSOR
    page_table = cast_rows.reshape(ROWS, N_TENSOR, shards).transpose(1, 0, 2).reshape(N_TENSOR, PAGES, 128)
    starts = jnp.cumsum(save_pages).astype(jnp.int32) - save_pages
    ranges = jnp.arange(ISLANDS, dtype=jnp.int32)
    inverse = jnp.zeros((ISLANDS,), jnp.int32).at[writer].set(ranges)
    slot_ids = jnp.arange(CAP, dtype=jnp.int32)
    page_index = starts[inverse][:, None] + slot_ids[None, :]
    is_valid = slot_ids[None, :] < save_pages[inverse][:, None]
    page_index = jnp.clip(page_index, 0, PAGES - 1).astype(jnp.int32)
    picked = page_table[:, page_index]
    picked = jnp.where(is_valid[None, :, :, None], picked, jnp.zeros_like(picked))
    checkpoint = picked.transpose(1, 2, 0, 3).reshape(ISLANDS, CAP, N_TENSOR * 128)
    return (new_master, new_momentum, checkpoint)
```

```python
import functools

import jax
import jax.numpy as jnp
from jax import lax
from jax.experimental import pallas as pl
from jax.experimental.pallas import tpu as pltpu
from jax.sharding import PartitionSpec as P

epsilon = 1e-06
decay_rate = 0.9
outer_rate = 0.7
LANES = 128
ROUNDS = 3
GATHER_ROUNDS = 2
MESH = pl.DeviceIdType.MESH


def cuts(total, unit, count):
    units = -(-total // unit)
    count = min(count, units)
    edges = [min(total, unit * (units * i // count)) for i in range(count + 1)]
    return [(edges[i], edges[i + 1] - edges[i]) for i in range(count)]


def bit_orders(bits):
    base = list(range(bits))
    orders = []
    for lead in range(min(3, bits)):
        orders.append([lead] + [b for b in base if b != lead])
    return orders


def at(bits_left, fixed, span):
    return tuple(fixed.get(b, slice(None)) for b in bits_left) + (pl.ds(*span), slice(None))


def kernel(bits, tensor, entries, x_ref, par_ref, mom_ref, master_ref, moment_ref, pages_ref, *scratch):
    acc = [x_ref] + list(scratch[:bits])
    sums, gathered, hi_sq, lo_sq = scratch[bits : bits + 4]
    rs_send, rs_recv, ag_send, ag_recv, hi_send, hi_recv, lo_send, lo_recv, out_sem = scratch[bits + 4 :]
    page_count = par_ref.shape[0]
    islands = 1 << bits
    me = lax.axis_index("island")
    my_t = lax.axis_index("tensor")
    mine = [lax.rem(me // (1 << b), 2) for b in range(bits)]
    partner = [me + (1 - 2 * mine[b]) * (1 << b) for b in range(bits)]
    all_bits = list(range(bits - 1, -1, -1))
    low_bits = bits // 2
    n_lo, n_hi = 1 << low_bits, 1 << (bits - low_bits)

    def flip(value, mask, width):
        out = value
        for b in range(width):
            if mask >> b & 1:
                out = out + (1 - 2 * lax.rem(value // (1 << b), 2)) * (1 << b)
        return out

    hi_peers = [(k, {"island": flip(me, k * n_lo, bits)}) for k in range(1, n_hi)]
    t_bits = tensor.bit_length() - 1
    lo_peers = []
    for k in range(1, n_lo * tensor):
        k_lo, k_t = k // tensor, k % tensor
        lo_peers.append((k, {"island": flip(me, k_lo, bits), "tensor": flip(my_t, k_t, t_bits)}))

    barrier = pltpu.get_barrier_semaphore()
    for _, peer in hi_peers + lo_peers:
        pl.semaphore_signal(barrier, inc=1, device_id=peer, device_id_type=MESH)
    pl.semaphore_wait(barrier, len(hi_peers) + len(lo_peers))

    orders = bit_orders(bits)
    spans = cuts(page_count, 8, len(orders) * ROUNDS)

    def left(c, s):
        used = orders[c % len(orders)][:s]
        return [b for b in all_bits if b not in used]

    def rs_copy(c, s):
        d = orders[c % len(orders)][s - 1]
        return pltpu.make_async_remote_copy(
            src_ref=acc[s - 1].at[at(left(c, s - 1), {d: 1 - mine[d]}, spans[c])],
            dst_ref=acc[s].at[at(left(c, s), {}, spans[c])],
            send_sem=rs_send.at[c, s - 1],
            recv_sem=rs_recv.at[c, s - 1],
            device_id={"island": partner[d]},
            device_id_type=MESH,
        )

    copies = {}
    for c in range(len(spans)):
        copies[c, 1] = rs_copy(c, 1)
        copies[c, 1].start()

    def when(item):
        c, s = item
        r = c // len(orders)
        return (0.1 * r if s == 1 else 1.1 * s + r, c)

    steps = sorted(((c, s) for c in range(len(spans)) for s in range(1, bits + 1)), key=when)
    for c, s in steps:
        order = orders[c % len(orders)]
        d = order[s - 1]
        copies[c, s].wait_recv()
        if s == bits:
            total = acc[s][at([], {}, spans[c])] + acc[s - 1][at(left(c, s - 1), {d: mine[d]}, spans[c])]
            sums[pl.ds(*spans[c]), :] = total * (1.0 / islands)
            continue
        e = order[s]
        for side in (1 - mine[e], mine[e]):
            to = at(left(c, s), {e: side}, spans[c])
            of = at(left(c, s - 1), {d: mine[d], e: side}, spans[c])
            acc[s][to] = acc[s][to] + acc[s - 1][of]
            if (c, s + 1) not in copies:
                copies[c, s + 1] = rs_copy(c, s + 1)
                copies[c, s + 1].start()

    grad = sums[...]
    hi_sq[0] = jnp.sum((grad * grad).reshape(page_count // 8, 8, LANES), axis=0)

    def exchange(box, peers, send, recv):
        sent = []
        for k, peer in peers:
            copy = pltpu.make_async_remote_copy(
                src_ref=box.at[0],
                dst_ref=box.at[k],
                send_sem=send.at[k],
                recv_sem=recv.at[k],
                device_id=peer,
                device_id_type=MESH,
            )
            copy.start()
            sent.append(copy)
        for copy in sent:
            copy.wait_recv()
        return sent

    sent = exchange(hi_sq, hi_peers, hi_send, hi_recv)
    lo_sq[0] = jnp.sum(hi_sq[...], axis=0)
    sent += exchange(lo_sq, lo_peers, lo_send, lo_recv)
    square_sum = jnp.sum(jnp.sum(lo_sq[...], axis=0), keepdims=True)
    norm = jnp.sqrt(square_sum / entries + epsilon)
    normed = grad / norm
    moment = decay_rate * mom_ref[...] + normed
    master = par_ref[...] - outer_rate * (normed + decay_rate * moment)
    gathered[tuple(mine[b] for b in all_bits)] = master.astype(jnp.bfloat16)

    ag_spans = cuts(page_count, 16, len(orders) * GATHER_ROUNDS)

    def ag_copy(c, s):
        order = orders[c % len(orders)][::-1]
        held = order[:s]
        where = at(all_bits, {b: mine[b] for b in all_bits if b not in held}, ag_spans[c])
        return pltpu.make_async_remote_copy(
            src_ref=gathered.at[where],
            dst_ref=gathered.at[where],
            send_sem=ag_send.at[c, s],
            recv_sem=ag_recv.at[c, s],
            device_id={"island": partner[order[s]]},
            device_id_type=MESH,
        )

    ag = {}
    for c in range(len(ag_spans)):
        ag[c, 0] = ag_copy(c, 0)
        ag[c, 0].start()
    moment_ref[...] = moment
    master_ref[...] = master
    for s in range(bits):
        for c in range(len(ag_spans)):
            ag[c, s].wait_recv()
            if s + 1 < bits:
                ag[c, s + 1] = ag_copy(c, s + 1)
                ag[c, s + 1].start()

    outs = []
    for i in range(islands):
        copy = pltpu.make_async_copy(
            gathered.at[tuple(i >> b & 1 for b in all_bits)], pages_ref.at[i], out_sem.at[i]
        )
        copy.start()
        outs.append(copy)
    for copy in list(copies.values()) + list(ag.values()) + sent:
        copy.wait_send()
    for copy in outs:
        copy.wait()


def body(islands, tensor, pseudo_grad, outer_params, momentum, save_pages, writer):
    own_rows, col_width = outer_params.shape
    bits = islands.bit_length() - 1
    page_count = own_rows * col_width // LANES
    capacity = 2 * page_count
    my_index = lax.axis_index("island")
    entries = islands * own_rows * col_width * tensor
    x = pseudo_grad.reshape((2,) * bits + (page_count, LANES))
    f32, bf16 = jnp.float32, jnp.bfloat16
    orders = len(bit_orders(bits))
    n_rs = len(cuts(page_count, 8, orders * ROUNDS))
    n_ag = len(cuts(page_count, 16, orders * GATHER_ROUNDS))
    n_lo = 1 << (bits // 2)
    n_hi = islands // n_lo
    dma = pltpu.SemaphoreType.DMA
    vmem = pl.BlockSpec(memory_space=pltpu.VMEM)
    spare = -(-capacity // page_count)
    master, moment, pages = pl.pallas_call(
        functools.partial(kernel, bits, tensor, entries),
        out_shape=(
            jax.ShapeDtypeStruct((page_count, LANES), f32),
            jax.ShapeDtypeStruct((page_count, LANES), f32),
            jax.ShapeDtypeStruct((islands + spare, page_count, LANES), bf16),
        ),
        in_specs=[vmem] * 3,
        out_specs=(vmem, vmem, pl.BlockSpec(memory_space=pl.ANY)),
        scratch_shapes=[pltpu.VMEM((2,) * (bits - s) + (page_count, LANES), f32) for s in range(1, bits + 1)]
        + [
            pltpu.VMEM((page_count, LANES), f32),
            pltpu.VMEM((2,) * bits + (page_count, LANES), bf16),
            pltpu.VMEM((n_hi, 8, LANES), f32),
            pltpu.VMEM((n_lo * tensor, 8, LANES), f32),
            dma((n_rs, bits)),
            dma((n_rs, bits)),
            dma((n_ag, bits)),
            dma((n_ag, bits)),
            dma((n_hi,)),
            dma((n_hi,)),
            dma((n_lo * tensor,)),
            dma((n_lo * tensor,)),
            dma((islands,)),
        ],
        compiler_params=pltpu.CompilerParams(collective_id=0, has_side_effects=True),
    )(x, outer_params.reshape(page_count, LANES), momentum.reshape(page_count, LANES))

    starts = jnp.cumsum(save_pages) - save_pages
    is_mine = writer == my_index
    own_start = jnp.sum(jnp.where(is_mine, starts, 0))
    own_length = jnp.sum(jnp.where(is_mine, save_pages, 0))
    pages = pages.reshape(-1, LANES)
    window = lax.dynamic_slice_in_dim(pages, own_start, capacity, 0)
    live = jnp.arange(capacity, dtype=jnp.int32) < own_length
    packed = jnp.where(live[:, None], window, jnp.zeros_like(window))
    shape = (own_rows, col_width)
    return master.reshape(shape), moment.reshape(shape), packed[None]


def solution(mesh):
    in_specs = (P("island", None, "tensor"), P("island", "tensor"), P("island", "tensor"), P(), P())
    out_specs = (P("island", "tensor"), P("island", "tensor"), P("island", None, "tensor"))
    step = functools.partial(body, mesh.shape["island"], mesh.shape["tensor"])
    return jax.shard_map(step, mesh=mesh, in_specs=in_specs, out_specs=out_specs, check_vma=False)
```

```python
import functools

import jax
import jax.numpy as jnp
from jax import lax
from jax.experimental import pallas as pl
from jax.experimental.pallas import tpu as pltpu
from jax.sharding import PartitionSpec as P

epsilon = 1e-06
decay_rate = 0.9
outer_rate = 0.7
LANES = 128
SUBLANES = 8
ROUNDS = 3
GATHER_CHUNKS = 2
MESH = pl.DeviceIdType.MESH


def cuts(total, unit, count):
    units = -(-total // unit)
    count = min(count, units)
    edges = [min(total, unit * (units * i // count)) for i in range(count + 1)]
    return [(edges[i], edges[i + 1] - edges[i]) for i in range(count)]


def bit_orders(bits):
    base = list(range(bits))
    orders = []
    for lead in range(min(3, bits)):
        orders.append([lead] + [b for b in base if b != lead])
    return orders


def at(bits_left, fixed, span):
    return tuple(fixed.get(b, slice(None)) for b in bits_left) + (pl.ds(*span), slice(None))


def flip(value, mask, width):
    out = value
    for b in range(width):
        if mask >> b & 1:
            out = out + (1 - 2 * lax.rem(value // (1 << b), 2)) * (1 << b)
    return out


def kernel(bits, tensor, rows, entries, *refs):
    x_ref, par_ref, mom_ref, save_ref, writer_ref, master_ref, moment_ref, pack_ref = refs[:8]
    scratch = refs[8:]
    page_count = par_ref.shape[0]
    capacity = pack_ref.shape[0]
    g_spans = cuts(page_count, 16, GATHER_CHUNKS)
    n_g = len(g_spans)
    acc = [x_ref] + list(scratch[:bits])
    held, parcel, landed = (scratch[bits + i * n_g : bits + (i + 1) * n_g] for i in range(3))
    scratch = scratch[bits + 3 * n_g :]
    sums, flat, span_buf, squares = scratch[:4]
    rs_send, rs_recv, sq_send, sq_recv, line_send, line_recv, del_send, del_recv = scratch[4:]
    islands = 1 << bits
    me = lax.axis_index("island")
    my_t = lax.axis_index("tensor")
    mine = [lax.rem(me // (1 << b), 2) for b in range(bits)]
    partner = [me + (1 - 2 * mine[b]) * (1 << b) for b in range(bits)]
    all_bits = list(range(bits - 1, -1, -1))
    n_lo = 1 << (bits // 2)
    n_hi = islands // n_lo
    my_hi, my_lo = me // n_lo, lax.rem(me, n_lo)

    t_bits = tensor.bit_length() - 1
    peers = []
    for k in range(1, islands * tensor):
        peers.append((k, {"island": flip(me, k // tensor, bits), "tensor": flip(my_t, k % tensor, t_bits)}))

    barrier = pltpu.get_barrier_semaphore()
    for _, peer in peers:
        pl.semaphore_signal(barrier, inc=1, device_id=peer, device_id_type=MESH)
    pl.semaphore_wait(barrier, len(peers))

    orders = bit_orders(bits)
    spans = cuts(page_count, 8, len(orders) * ROUNDS)

    def left(c, s):
        used = orders[c % len(orders)][:s]
        return [b for b in all_bits if b not in used]

    def rs_copy(c, s):
        d = orders[c % len(orders)][s - 1]
        return pltpu.make_async_remote_copy(
            src_ref=acc[s - 1].at[at(left(c, s - 1), {d: 1 - mine[d]}, spans[c])],
            dst_ref=acc[s].at[at(left(c, s), {}, spans[c])],
            send_sem=rs_send.at[c, s - 1],
            recv_sem=rs_recv.at[c, s - 1],
            device_id={"island": partner[d]},
            device_id_type=MESH,
        )

    copies = {}
    for c in range(len(spans)):
        copies[c, 1] = rs_copy(c, 1)
        copies[c, 1].start()

    def when(item):
        c, s = item
        r = c // len(orders)
        return (0.1 * r if s == 1 else 1.1 * s + r, c)

    steps = sorted(((c, s) for c in range(len(spans)) for s in range(1, bits + 1)), key=when)
    for c, s in steps:
        order = orders[c % len(orders)]
        d = order[s - 1]
        copies[c, s].wait_recv()
        if s == bits:
            total = acc[s][at([], {}, spans[c])] + acc[s - 1][at(left(c, s - 1), {d: mine[d]}, spans[c])]
            sums[pl.ds(*spans[c]), :] = total * (1.0 / islands)
            continue
        e = order[s]
        for side in (1 - mine[e], mine[e]):
            to = at(left(c, s), {e: side}, spans[c])
            of = at(left(c, s - 1), {d: mine[d], e: side}, spans[c])
            acc[s][to] = acc[s][to] + acc[s - 1][of]
            if (c, s + 1) not in copies:
                copies[c, s + 1] = rs_copy(c, s + 1)
                copies[c, s + 1].start()

    starts, running = [], jnp.int32(0)
    for k in range(islands):
        starts.append(running)
        running = running + save_ref[k]

    def range_of(island):
        start, length = jnp.int32(0), jnp.int32(0)
        for k in range(islands):
            hit = writer_ref[k] == island
            start = start + jnp.where(hit, starts[k], 0)
            length = length + jnp.where(hit, save_ref[k], 0)
        return start, length

    wanted = [range_of(flip(me, k, bits)) for k in range(n_lo)]
    first_block = [lax.div(start, jnp.int32(page_count)) for start, _ in wanted]

    grad = sums[...]
    squares[0] = jnp.sum((grad * grad).reshape(page_count // 8, 8, LANES), axis=0)
    sent = []
    for k, peer in peers:
        copy = pltpu.make_async_remote_copy(
            src_ref=squares.at[0],
            dst_ref=squares.at[k],
            send_sem=sq_send.at[k],
            recv_sem=sq_recv.at[k],
            device_id=peer,
            device_id_type=MESH,
        )
        copy.start()
        sent.append(copy)
    for copy in sent:
        copy.wait_recv()
    square_sum = jnp.sum(jnp.sum(squares[...], axis=0), keepdims=True)
    norm = jnp.sqrt(square_sum / entries + epsilon)
    normed = grad / norm
    moment = decay_rate * mom_ref[...] + normed
    master = par_ref[...] - outer_rate * (normed + decay_rate * moment)
    master_ref[...] = master
    moment_ref[...] = moment
    tiles = page_count // rows
    for r in range(rows):
        flat[pl.ds(r * tiles, tiles), :] = master_ref[pl.ds(r, tiles, stride=rows), :]
    for g, span in enumerate(g_spans):
        held[g][my_hi] = flat[pl.ds(*span), :].astype(jnp.bfloat16)

    def line(g, way, step):
        block = my_hi - step if way == 0 else my_hi + step
        return pltpu.make_async_remote_copy(
            src_ref=held[g].at[block],
            dst_ref=held[g].at[block],
            send_sem=line_send.at[g, way, step],
            recv_sem=line_recv.at[g, way, step],
            device_id={"island": me + n_lo if way == 0 else me - n_lo},
            device_id_type=MESH,
        )

    def sends(way, step):
        if way == 0:
            return jnp.logical_and(my_hi >= step, my_hi < n_hi - 1)
        return jnp.logical_and(my_hi <= n_hi - 1 - step, my_hi > 0)

    def arrives(way, step):
        return my_hi > step if way == 0 else my_hi < n_hi - 1 - step

    def start_line(g, way, step):
        pl.when(sends(way, step))(lambda: line(g, way, step).start())

    def end_line(g, way, step):
        def wait():
            block = my_hi - 1 - step if way == 0 else my_hi + 1 + step
            pltpu.make_async_remote_copy(
                src_ref=held[g].at[block],
                dst_ref=held[g].at[block],
                send_sem=line_send.at[g, way, step],
                recv_sem=line_recv.at[g, way, step],
                device_id={"island": me},
                device_id_type=MESH,
            ).wait_recv()

        pl.when(arrives(way, step))(wait)

    for g in range(n_g):
        for way in range(2):
            start_line(g, way, 0)
    parcels = []
    for g in range(n_g):
        for step in range(n_hi - 1):
            for way in range(2):
                end_line(g, way, step)
                if step + 1 < n_hi - 1:
                    start_line(g, way, step + 1)
        for k in range(n_lo - 1, -1, -1):
            ahead = lax.rem(my_lo + islands - first_block[k], jnp.int32(n_lo))
            which = lax.div(jnp.minimum(first_block[k] + ahead, islands - 1), jnp.int32(n_lo))
            if k == 0:
                landed[g][0] = held[g][which]
                continue
            parcel[g][k] = held[g][which]
            copy = pltpu.make_async_remote_copy(
                src_ref=parcel[g].at[k],
                dst_ref=landed[g].at[k],
                send_sem=del_send.at[g, k],
                recv_sem=del_recv.at[g, k],
                device_id={"island": flip(me, k, bits)},
                device_id_type=MESH,
            )
            copy.start()
            parcels.append(copy)
    spread = span_buf.shape[0] // page_count
    for g, (low, size) in enumerate(g_spans):
        for copy in parcels[g * (n_lo - 1) : (g + 1) * (n_lo - 1)]:
            copy.wait_recv()
        for m in range(spread):
            slot = lax.rem(first_block[0] + m, jnp.int32(n_lo)) ^ my_lo
            span_buf[pl.ds(m * page_count + low, size), :] = landed[g][slot].astype(jnp.float32)
    start, length = wanted[0]
    window = span_buf[pl.ds(start - first_block[0] * page_count, capacity), :]
    live = lax.broadcasted_iota(jnp.int32, window.shape, 0) < length
    pack_ref[...] = jnp.where(live, window, 0.0).astype(jnp.bfloat16)

    for copy in list(copies.values()) + parcels + sent:
        copy.wait_send()
    for g in range(n_g):
        for way in range(2):
            for step in range(n_hi - 1):
                pl.when(sends(way, step))(lambda g=g, way=way, step=step: line(g, way, step).wait_send())


def body(islands, tensor, pseudo_grad, outer_params, momentum, save_pages, writer):
    own_rows, col_width = outer_params.shape
    bits = islands.bit_length() - 1
    tiles = col_width // LANES
    page_count = own_rows * tiles
    capacity = 2 * page_count
    entries = islands * own_rows * col_width * tensor
    f32, bf16 = jnp.float32, jnp.bfloat16
    n_rs = len(cuts(page_count, 8, len(bit_orders(bits)) * ROUNDS))
    g_spans = cuts(page_count, 16, GATHER_CHUNKS)
    n_g = len(g_spans)
    n_lo = 1 << (bits // 2)
    n_hi = islands // n_lo
    dma = pltpu.SemaphoreType.DMA
    vmem = pl.BlockSpec(memory_space=pltpu.VMEM)
    smem = pl.BlockSpec(memory_space=pltpu.SMEM)

    def interleave(a):
        return a.reshape(-1, own_rows, tiles, LANES).swapaxes(1, 2).reshape(-1, page_count, LANES)

    def rows_of(a):
        return a.reshape(tiles, own_rows, LANES).swapaxes(0, 1).reshape(own_rows, col_width)

    x = pseudo_grad.reshape(-1, SUBLANES, tiles, LANES).swapaxes(1, 2)
    x = x.reshape(-1, tiles, SUBLANES // own_rows, own_rows, LANES).swapaxes(1, 2)
    x = x.reshape((2,) * bits + (page_count, LANES))
    master, moment, packed = pl.pallas_call(
        functools.partial(kernel, bits, tensor, own_rows, entries),
        out_shape=(
            jax.ShapeDtypeStruct((page_count, LANES), f32),
            jax.ShapeDtypeStruct((page_count, LANES), f32),
            jax.ShapeDtypeStruct((capacity, LANES), bf16),
        ),
        in_specs=[vmem] * 3 + [smem] * 2,
        out_specs=(vmem,) * 3,
        scratch_shapes=[pltpu.VMEM((2,) * (bits - s) + (page_count, LANES), f32) for s in range(1, bits + 1)]
        + [pltpu.VMEM((n_hi, size, LANES), bf16) for _, size in g_spans]
        + [pltpu.VMEM((n_lo, size, LANES), bf16) for _, size in g_spans]
        + [pltpu.VMEM((n_lo, size, LANES), bf16) for _, size in g_spans]
        + [
            pltpu.VMEM((page_count, LANES), f32),
            pltpu.VMEM((page_count, LANES), f32),
            pltpu.VMEM((capacity + page_count, LANES), f32),
            pltpu.VMEM((islands * tensor, 8, LANES), f32),
            dma((n_rs, bits)),
            dma((n_rs, bits)),
            dma((islands * tensor,)),
            dma((islands * tensor,)),
            dma((n_g, 2, n_hi)),
            dma((n_g, 2, n_hi)),
            dma((n_g, n_lo)),
            dma((n_g, n_lo)),
        ],
        compiler_params=pltpu.CompilerParams(collective_id=0, has_side_effects=True),
    )(x, interleave(outer_params)[0], interleave(momentum)[0], save_pages, writer)
    return rows_of(master), rows_of(moment), packed[None]


def solution(mesh):
    in_specs = (P("island", None, "tensor"), P("island", "tensor"), P("island", "tensor"), P(), P())
    out_specs = (P("island", "tensor"), P("island", "tensor"), P("island", None, "tensor"))
    step = functools.partial(body, mesh.shape["island"], mesh.shape["tensor"])
    return jax.shard_map(step, mesh=mesh, in_specs=in_specs, out_specs=out_specs, check_vma=False)
```

```python
import functools

import jax
import jax.numpy as jnp
from jax import lax
from jax.experimental import pallas as pl
from jax.experimental.pallas import tpu as pltpu
from jax.sharding import PartitionSpec as P

epsilon = 1e-06
decay_rate = 0.9
outer_rate = 0.7
LANES = 128
SUBLANES = 8
ROUNDS = 3
GATHER_CHUNKS = 2
MESH = pl.DeviceIdType.MESH


def cuts(total, unit, count):
    units = -(-total // unit)
    count = min(count, units)
    edges = [min(total, unit * (units * i // count)) for i in range(count + 1)]
    return [(edges[i], edges[i + 1] - edges[i]) for i in range(count)]


def bit_orders(bits):
    base = list(range(bits))
    orders = []
    for lead in range(min(3, bits)):
        orders.append([lead] + [b for b in base if b != lead])
    return orders


def at(bits_left, fixed, span):
    return tuple(fixed.get(b, slice(None)) for b in bits_left) + (pl.ds(*span), slice(None))


def flip(value, mask, width):
    out = value
    for b in range(width):
        if mask >> b & 1:
            out = out + (1 - 2 * lax.rem(value // (1 << b), 2)) * (1 << b)
    return out


def kernel(bits, tensor, rows, entries, *refs):
    x_ref, par_ref, mom_ref, save_ref, writer_ref, master_ref, moment_ref, pack_ref = refs[:8]
    scratch = refs[8:]
    page_count = par_ref.shape[0]
    capacity = pack_ref.shape[0]
    g_spans = cuts(page_count, 16, GATHER_CHUNKS)
    n_g = len(g_spans)
    raw, acc = scratch[0], scratch[1 : bits + 2]
    scratch = scratch[1:]
    scratch = scratch[bits + 1 :]
    held, parcel, landed = (scratch[i * n_g : (i + 1) * n_g] for i in range(3))
    scratch = scratch[3 * n_g :]
    sums, flat, span_buf, squares = scratch[:4]
    rs_send, rs_recv, sq_send, sq_recv, line_send, line_recv, del_send, del_recv, in_sem = scratch[4:]
    islands = 1 << bits
    me = lax.axis_index("island")
    my_t = lax.axis_index("tensor")
    mine = [lax.rem(me // (1 << b), 2) for b in range(bits)]
    partner = [me + (1 - 2 * mine[b]) * (1 << b) for b in range(bits)]
    all_bits = list(range(bits - 1, -1, -1))
    n_lo = 1 << (bits // 2)
    n_hi = islands // n_lo
    my_hi, my_lo = me // n_lo, lax.rem(me, n_lo)

    t_bits = tensor.bit_length() - 1
    peers = []
    for k in range(1, islands * tensor):
        peers.append((k, {"island": flip(me, k // tensor, bits), "tensor": flip(my_t, k % tensor, t_bits)}))

    orders = bit_orders(bits)
    spans = cuts(page_count, SUBLANES, len(orders) * ROUNDS)
    loads = []
    for c, (low, size) in enumerate(spans):
        part = pl.ds(low // rows * SUBLANES, size // rows * SUBLANES)
        loads.append(pltpu.make_async_copy(x_ref.at[:, part, :], raw.at[:, part, :], in_sem.at[c]))
        loads[c].start()

    barrier = pltpu.get_barrier_semaphore()
    for _, peer in peers:
        pl.semaphore_signal(barrier, inc=1, device_id=peer, device_id_type=MESH)

    def lay_out(c):
        low, size = spans[c]
        loads[c].wait()
        for i in range(islands):
            group, first = i * rows // SUBLANES, i * rows % SUBLANES
            for r in range(rows):
                line = raw[group, pl.ds(low // rows * SUBLANES + first + r, size // rows, stride=SUBLANES), :]
                to = tuple(i >> b & 1 for b in all_bits)
                acc[0][to + (pl.ds(low + r, size // rows, stride=rows), slice(None))] = line

    for c in range(len(orders)):
        lay_out(c)
    pl.semaphore_wait(barrier, len(peers))

    def left(c, s):
        used = orders[c % len(orders)][:s]
        return [b for b in all_bits if b not in used]

    def rs_copy(c, s):
        d = orders[c % len(orders)][s - 1]
        return pltpu.make_async_remote_copy(
            src_ref=acc[s - 1].at[at(left(c, s - 1), {d: 1 - mine[d]}, spans[c])],
            dst_ref=acc[s].at[at(left(c, s), {}, spans[c])],
            send_sem=rs_send.at[c, s - 1],
            recv_sem=rs_recv.at[c, s - 1],
            device_id={"island": partner[d]},
            device_id_type=MESH,
        )

    copies = {}
    for c in range(len(spans)):
        if c >= len(orders):
            lay_out(c)
        copies[c, 1] = rs_copy(c, 1)
        copies[c, 1].start()

    def when(item):
        c, s = item
        r = c // len(orders)
        return (0.1 * r if s == 1 else 1.1 * s + r, c)

    steps = sorted(((c, s) for c in range(len(spans)) for s in range(1, bits + 1)), key=when)
    for c, s in steps:
        order = orders[c % len(orders)]
        d = order[s - 1]
        copies[c, s].wait_recv()
        if s == bits:
            total = acc[s][at([], {}, spans[c])] + acc[s - 1][at(left(c, s - 1), {d: mine[d]}, spans[c])]
            sums[pl.ds(*spans[c]), :] = total * (1.0 / islands)
            continue
        e = order[s]
        for side in (1 - mine[e], mine[e]):
            to = at(left(c, s), {e: side}, spans[c])
            of = at(left(c, s - 1), {d: mine[d], e: side}, spans[c])
            acc[s][to] = acc[s][to] + acc[s - 1][of]
            if (c, s + 1) not in copies:
                copies[c, s + 1] = rs_copy(c, s + 1)
                copies[c, s + 1].start()

    starts, running = [], jnp.int32(0)
    for k in range(islands):
        starts.append(running)
        running = running + save_ref[k]

    def range_of(island):
        start, length = jnp.int32(0), jnp.int32(0)
        for k in range(islands):
            hit = writer_ref[k] == island
            start = start + jnp.where(hit, starts[k], 0)
            length = length + jnp.where(hit, save_ref[k], 0)
        return start, length

    wanted = [range_of(flip(me, k, bits)) for k in range(n_lo)]
    first_block = [lax.div(start, jnp.int32(page_count)) for start, _ in wanted]

    grad = sums[...]
    squares[0] = jnp.sum((grad * grad).reshape(page_count // 8, 8, LANES), axis=0)
    sent = []
    for k, peer in peers:
        copy = pltpu.make_async_remote_copy(
            src_ref=squares.at[0],
            dst_ref=squares.at[k],
            send_sem=sq_send.at[k],
            recv_sem=sq_recv.at[k],
            device_id=peer,
            device_id_type=MESH,
        )
        copy.start()
        sent.append(copy)
    for copy in sent:
        copy.wait_recv()
    square_sum = jnp.sum(jnp.sum(squares[...], axis=0), keepdims=True)
    norm = jnp.sqrt(square_sum / entries + epsilon)
    normed = grad / norm
    moment = decay_rate * mom_ref[...] + normed
    master = par_ref[...] - outer_rate * (normed + decay_rate * moment)
    master_ref[...] = master
    moment_ref[...] = moment
    tiles = page_count // rows
    for r in range(rows):
        flat[pl.ds(r * tiles, tiles), :] = master_ref[pl.ds(r, tiles, stride=rows), :]
    for g, span in enumerate(g_spans):
        held[g][my_hi] = flat[pl.ds(*span), :].astype(jnp.bfloat16)

    def line(g, way, step):
        block = my_hi - step if way == 0 else my_hi + step
        return pltpu.make_async_remote_copy(
            src_ref=held[g].at[block],
            dst_ref=held[g].at[block],
            send_sem=line_send.at[g, way, step],
            recv_sem=line_recv.at[g, way, step],
            device_id={"island": me + n_lo if way == 0 else me - n_lo},
            device_id_type=MESH,
        )

    def sends(way, step):
        if way == 0:
            return jnp.logical_and(my_hi >= step, my_hi < n_hi - 1)
        return jnp.logical_and(my_hi <= n_hi - 1 - step, my_hi > 0)

    def arrives(way, step):
        return my_hi > step if way == 0 else my_hi < n_hi - 1 - step

    def start_line(g, way, step):
        pl.when(sends(way, step))(lambda: line(g, way, step).start())

    def end_line(g, way, step):
        def wait():
            block = my_hi - 1 - step if way == 0 else my_hi + 1 + step
            pltpu.make_async_remote_copy(
                src_ref=held[g].at[block],
                dst_ref=held[g].at[block],
                send_sem=line_send.at[g, way, step],
                recv_sem=line_recv.at[g, way, step],
                device_id={"island": me},
                device_id_type=MESH,
            ).wait_recv()

        pl.when(arrives(way, step))(wait)

    for g in range(n_g):
        for way in range(2):
            start_line(g, way, 0)
    parcels = []
    for g in range(n_g):
        for step in range(n_hi - 1):
            for way in range(2):
                end_line(g, way, step)
                if step + 1 < n_hi - 1:
                    start_line(g, way, step + 1)
        for k in range(n_lo - 1, -1, -1):
            ahead = lax.rem(my_lo + islands - first_block[k], jnp.int32(n_lo))
            which = lax.div(jnp.minimum(first_block[k] + ahead, islands - 1), jnp.int32(n_lo))
            if k == 0:
                landed[g][0] = held[g][which]
                continue
            parcel[g][k] = held[g][which]
            copy = pltpu.make_async_remote_copy(
                src_ref=parcel[g].at[k],
                dst_ref=landed[g].at[k],
                send_sem=del_send.at[g, k],
                recv_sem=del_recv.at[g, k],
                device_id={"island": flip(me, k, bits)},
                device_id_type=MESH,
            )
            copy.start()
            parcels.append(copy)
    spread = span_buf.shape[0] // page_count
    for g, (low, size) in enumerate(g_spans):
        for copy in parcels[g * (n_lo - 1) : (g + 1) * (n_lo - 1)]:
            copy.wait_recv()
        for m in range(spread):
            slot = lax.rem(first_block[0] + m, jnp.int32(n_lo)) ^ my_lo
            span_buf[pl.ds(m * page_count + low, size), :] = landed[g][slot].astype(jnp.float32)
    start, length = wanted[0]
    window = span_buf[pl.ds(start - first_block[0] * page_count, capacity), :]
    live = lax.broadcasted_iota(jnp.int32, window.shape, 0) < length
    pack_ref[...] = jnp.where(live, window, 0.0).astype(jnp.bfloat16)

    for copy in list(copies.values()) + parcels + sent:
        copy.wait_send()
    for g in range(n_g):
        for way in range(2):
            for step in range(n_hi - 1):
                pl.when(sends(way, step))(lambda g=g, way=way, step=step: line(g, way, step).wait_send())


def hand_on(*refs):
    for source, target in zip(refs[:3], refs[3:]):
        target[...] = source[...]


def body(islands, tensor, pseudo_grad, outer_params, momentum, save_pages, writer):
    own_rows, col_width = outer_params.shape
    bits = islands.bit_length() - 1
    tiles = col_width // LANES
    page_count = own_rows * tiles
    capacity = 2 * page_count
    entries = islands * own_rows * col_width * tensor
    f32, bf16 = jnp.float32, jnp.bfloat16
    n_rs = len(cuts(page_count, SUBLANES, len(bit_orders(bits)) * ROUNDS))
    g_spans = cuts(page_count, 16, GATHER_CHUNKS)
    n_g = len(g_spans)
    n_lo = 1 << (bits // 2)
    n_hi = islands // n_lo
    dma = pltpu.SemaphoreType.DMA
    vmem = pl.BlockSpec(memory_space=pltpu.VMEM)
    smem = pl.BlockSpec(memory_space=pltpu.SMEM)

    def interleave(a):
        return a.reshape(-1, own_rows, tiles, LANES).swapaxes(1, 2).reshape(-1, page_count, LANES)

    def rows_of(a):
        return a.reshape(tiles, own_rows, LANES).swapaxes(0, 1).reshape(own_rows, col_width)

    x = pseudo_grad.reshape(-1, SUBLANES, tiles, LANES).swapaxes(1, 2)
    x = x.reshape(-1, tiles * SUBLANES, LANES)
    master, moment, packed = pl.pallas_call(
        functools.partial(kernel, bits, tensor, own_rows, entries),
        out_shape=(
            jax.ShapeDtypeStruct((page_count, LANES), f32),
            jax.ShapeDtypeStruct((page_count, LANES), f32),
            jax.ShapeDtypeStruct((capacity, LANES), bf16),
        ),
        in_specs=[pl.BlockSpec(memory_space=pl.ANY)] + [vmem] * 2 + [smem] * 2,
        out_specs=(vmem,) * 3,
        scratch_shapes=[pltpu.VMEM(x.shape, f32)]
        + [pltpu.VMEM((2,) * (bits - s) + (page_count, LANES), f32) for s in range(bits + 1)]
        + [pltpu.VMEM((n_hi, size, LANES), bf16) for _, size in g_spans]
        + [pltpu.VMEM((n_lo, size, LANES), bf16) for _, size in g_spans]
        + [pltpu.VMEM((n_lo, size, LANES), bf16) for _, size in g_spans]
        + [
            pltpu.VMEM((page_count, LANES), f32),
            pltpu.VMEM((page_count, LANES), f32),
            pltpu.VMEM((capacity + page_count, LANES), f32),
            pltpu.VMEM((islands * tensor, 8, LANES), f32),
            dma((n_rs, bits)),
            dma((n_rs, bits)),
            dma((islands * tensor,)),
            dma((islands * tensor,)),
            dma((n_g, 2, n_hi)),
            dma((n_g, 2, n_hi)),
            dma((n_g, n_lo)),
            dma((n_g, n_lo)),
            dma((n_rs,)),
        ],
        compiler_params=pltpu.CompilerParams(collective_id=0, has_side_effects=True),
    )(x, interleave(outer_params)[0], interleave(momentum)[0], save_pages, writer)
    master, moment, packed = pl.pallas_call(
        hand_on,
        out_shape=tuple(jax.ShapeDtypeStruct(a.shape, a.dtype) for a in (master, moment, packed)),
        in_specs=[vmem] * 3,
        out_specs=(vmem,) * 3,
    )(master, moment, packed)
    return rows_of(master), rows_of(moment), packed[None]


def solution(mesh):
    in_specs = (P("island", None, "tensor"), P("island", "tensor"), P("island", "tensor"), P(), P())
    out_specs = (P("island", "tensor"), P("island", "tensor"), P("island", None, "tensor"))
    step = functools.partial(body, mesh.shape["island"], mesh.shape["tensor"])
    return jax.shard_map(step, mesh=mesh, in_specs=in_specs, out_specs=out_specs, check_vma=False)
```

```python
import functools

import jax
import jax.numpy as jnp
from jax import lax
from jax.experimental import pallas as pl
from jax.experimental.pallas import tpu as pltpu
from jax.sharding import PartitionSpec as P

epsilon = 1e-06
decay_rate = 0.9
outer_rate = 0.7
LANES = 128
SUBLANES = 8
ROUNDS = 2
GATHER_CHUNKS = 2
MESH = pl.DeviceIdType.MESH


def cuts(total, unit, count):
    units = -(-total // unit)
    count = min(count, units)
    edges = [min(total, unit * (units * i // count)) for i in range(count + 1)]
    return [(edges[i], edges[i + 1] - edges[i]) for i in range(count)]


def bit_orders(bits):
    base = list(range(bits))
    orders = []
    for lead in range(min(3, bits)):
        orders.append([lead] + [b for b in base if b != lead])
    if bits < 3:
        return orders
    return orders + orders[:2] + [[2, 1, 0] + base[3:]]


def at(bits_left, fixed, span):
    return tuple(fixed.get(b, slice(None)) for b in bits_left) + (pl.ds(*span), slice(None))


def flip(value, mask, width):
    out = value
    for b in range(width):
        if mask >> b & 1:
            out = out + (1 - 2 * lax.rem(value // (1 << b), 2)) * (1 << b)
    return out


def kernel(bits, tensor, rows, entries, *refs):
    x_ref, par_ref, mom_ref, save_ref, writer_ref, master_ref, moment_ref, pack_ref = refs[:8]
    scratch = refs[8:]
    page_count = par_ref.shape[0]
    capacity = pack_ref.shape[0]
    g_spans = cuts(page_count, 16, GATHER_CHUNKS)
    n_g = len(g_spans)
    raw, acc = scratch[0], scratch[1 : bits + 2]
    scratch = scratch[1:]
    scratch = scratch[bits + 1 :]
    held, parcel, landed = (scratch[i * n_g : (i + 1) * n_g] for i in range(3))
    scratch = scratch[3 * n_g :]
    sums, flat, span_buf, squares = scratch[:4]
    rs_send, rs_recv, sq_send, sq_recv, line_send, line_recv, del_send, del_recv, in_sem = scratch[4:]
    islands = 1 << bits
    me = lax.axis_index("island")
    my_t = lax.axis_index("tensor")
    mine = [lax.rem(me // (1 << b), 2) for b in range(bits)]
    partner = [me + (1 - 2 * mine[b]) * (1 << b) for b in range(bits)]
    all_bits = list(range(bits - 1, -1, -1))
    n_lo = 1 << (bits // 2)
    n_hi = islands // n_lo
    my_hi, my_lo = me // n_lo, lax.rem(me, n_lo)

    t_bits = tensor.bit_length() - 1
    peers = []
    for k in range(1, islands * tensor):
        peers.append((k, {"island": flip(me, k // tensor, bits), "tensor": flip(my_t, k % tensor, t_bits)}))

    orders = bit_orders(bits)
    spans = cuts(page_count, SUBLANES, len(orders) * ROUNDS)
    loads = []
    for c, (low, size) in enumerate(spans):
        part = pl.ds(low // rows * SUBLANES, size // rows * SUBLANES)
        loads.append(pltpu.make_async_copy(x_ref.at[:, part, :], raw.at[:, part, :], in_sem.at[c]))
        loads[c].start()

    barrier = pltpu.get_barrier_semaphore()
    for _, peer in peers:
        pl.semaphore_signal(barrier, inc=1, device_id=peer, device_id_type=MESH)

    def lay_out(c):
        low, size = spans[c]
        loads[c].wait()
        for i in range(islands):
            group, first = i * rows // SUBLANES, i * rows % SUBLANES
            for r in range(rows):
                line = raw[group, pl.ds(low // rows * SUBLANES + first + r, size // rows, stride=SUBLANES), :]
                to = tuple(i >> b & 1 for b in all_bits)
                acc[0][to + (pl.ds(low + r, size // rows, stride=rows), slice(None))] = line

    for c in range(3):
        lay_out(c)
    pl.semaphore_wait(barrier, len(peers))

    def left(c, s):
        used = orders[c % len(orders)][:s]
        return [b for b in all_bits if b not in used]

    def rs_copy(c, s):
        d = orders[c % len(orders)][s - 1]
        return pltpu.make_async_remote_copy(
            src_ref=acc[s - 1].at[at(left(c, s - 1), {d: 1 - mine[d]}, spans[c])],
            dst_ref=acc[s].at[at(left(c, s), {}, spans[c])],
            send_sem=rs_send.at[c, s - 1],
            recv_sem=rs_recv.at[c, s - 1],
            device_id={"island": partner[d]},
            device_id_type=MESH,
        )

    copies = {}
    for c in range(len(spans)):
        if c >= 3:
            lay_out(c)
        copies[c, 1] = rs_copy(c, 1)
        copies[c, 1].start()

    def when(item):
        c, s = item
        r = c // 3 * 0.75
        return (0.1 * r if s == 1 else 1.1 * s + r, c)

    steps = sorted(((c, s) for c in range(len(spans)) for s in range(1, bits + 1)), key=when)
    for c, s in steps:
        order = orders[c % len(orders)]
        d = order[s - 1]
        copies[c, s].wait_recv()
        if s == bits:
            total = acc[s][at([], {}, spans[c])] + acc[s - 1][at(left(c, s - 1), {d: mine[d]}, spans[c])]
            sums[pl.ds(*spans[c]), :] = total * (1.0 / islands)
            continue
        e = order[s]
        for side in (1 - mine[e], mine[e]):
            to = at(left(c, s), {e: side}, spans[c])
            of = at(left(c, s - 1), {d: mine[d], e: side}, spans[c])
            acc[s][to] = acc[s][to] + acc[s - 1][of]
            if (c, s + 1) not in copies:
                copies[c, s + 1] = rs_copy(c, s + 1)
                copies[c, s + 1].start()

    starts, running = [], jnp.int32(0)
    for k in range(islands):
        starts.append(running)
        running = running + save_ref[k]

    def range_of(island):
        start, length = jnp.int32(0), jnp.int32(0)
        for k in range(islands):
            hit = writer_ref[k] == island
            start = start + jnp.where(hit, starts[k], 0)
            length = length + jnp.where(hit, save_ref[k], 0)
        return start, length

    wanted = [range_of(flip(me, k, bits)) for k in range(n_lo)]
    first_block = [lax.div(start, jnp.int32(page_count)) for start, _ in wanted]

    grad = sums[...]
    squares[0] = jnp.sum((grad * grad).reshape(page_count // 8, 8, LANES), axis=0)
    sent = []
    for k, peer in peers:
        copy = pltpu.make_async_remote_copy(
            src_ref=squares.at[0],
            dst_ref=squares.at[k],
            send_sem=sq_send.at[k],
            recv_sem=sq_recv.at[k],
            device_id=peer,
            device_id_type=MESH,
        )
        copy.start()
        sent.append(copy)
    for copy in sent:
        copy.wait_recv()
    square_sum = jnp.sum(jnp.sum(squares[...], axis=0), keepdims=True)
    norm = jnp.sqrt(square_sum / entries + epsilon)
    normed = grad / norm
    moment = decay_rate * mom_ref[...] + normed
    master = par_ref[...] - outer_rate * (normed + decay_rate * moment)
    master_ref[...] = master
    moment_ref[...] = moment
    tiles = page_count // rows
    for r in range(rows):
        flat[pl.ds(r * tiles, tiles), :] = master_ref[pl.ds(r, tiles, stride=rows), :]
    for g, span in enumerate(g_spans):
        held[g][my_hi] = flat[pl.ds(*span), :].astype(jnp.bfloat16)

    def line(g, way, step):
        block = my_hi - step if way == 0 else my_hi + step
        return pltpu.make_async_remote_copy(
            src_ref=held[g].at[block],
            dst_ref=held[g].at[block],
            send_sem=line_send.at[g, way, step],
            recv_sem=line_recv.at[g, way, step],
            device_id={"island": me + n_lo if way == 0 else me - n_lo},
            device_id_type=MESH,
        )

    def sends(way, step):
        if way == 0:
            return jnp.logical_and(my_hi >= step, my_hi < n_hi - 1)
        return jnp.logical_and(my_hi <= n_hi - 1 - step, my_hi > 0)

    def arrives(way, step):
        return my_hi > step if way == 0 else my_hi < n_hi - 1 - step

    def start_line(g, way, step):
        pl.when(sends(way, step))(lambda: line(g, way, step).start())

    def end_line(g, way, step):
        def wait():
            block = my_hi - 1 - step if way == 0 else my_hi + 1 + step
            pltpu.make_async_remote_copy(
                src_ref=held[g].at[block],
                dst_ref=held[g].at[block],
                send_sem=line_send.at[g, way, step],
                recv_sem=line_recv.at[g, way, step],
                device_id={"island": me},
                device_id_type=MESH,
            ).wait_recv()

        pl.when(arrives(way, step))(wait)

    for g in range(n_g):
        for way in range(2):
            start_line(g, way, 0)
    parcels = []
    for g in range(n_g):
        for step in range(n_hi - 1):
            for way in range(2):
                end_line(g, way, step)
                if step + 1 < n_hi - 1:
                    start_line(g, way, step + 1)
        for k in range(n_lo - 1, -1, -1):
            ahead = lax.rem(my_lo + islands - first_block[k], jnp.int32(n_lo))
            which = lax.div(jnp.minimum(first_block[k] + ahead, islands - 1), jnp.int32(n_lo))
            if k == 0:
                landed[g][0] = held[g][which]
                continue
            parcel[g][k] = held[g][which]
            copy = pltpu.make_async_remote_copy(
                src_ref=parcel[g].at[k],
                dst_ref=landed[g].at[k],
                send_sem=del_send.at[g, k],
                recv_sem=del_recv.at[g, k],
                device_id={"island": flip(me, k, bits)},
                device_id_type=MESH,
            )
            copy.start()
            parcels.append(copy)
    spread = span_buf.shape[0] // page_count
    for g, (low, size) in enumerate(g_spans):
        for copy in parcels[g * (n_lo - 1) : (g + 1) * (n_lo - 1)]:
            copy.wait_recv()
        for m in range(spread):
            slot = lax.rem(first_block[0] + m, jnp.int32(n_lo)) ^ my_lo
            span_buf[pl.ds(m * page_count + low, size), :] = landed[g][slot].astype(jnp.float32)
    start, length = wanted[0]
    window = span_buf[pl.ds(start - first_block[0] * page_count, capacity), :]
    live = lax.broadcasted_iota(jnp.int32, window.shape, 0) < length
    pack_ref[...] = jnp.where(live, window, 0.0).astype(jnp.bfloat16)

    for copy in list(copies.values()) + parcels + sent:
        copy.wait_send()
    for g in range(n_g):
        for way in range(2):
            for step in range(n_hi - 1):
                pl.when(sends(way, step))(lambda g=g, way=way, step=step: line(g, way, step).wait_send())


def hand_on(*refs):
    for source, target in zip(refs[:3], refs[3:]):
        target[...] = source[...]


def body(islands, tensor, pseudo_grad, outer_params, momentum, save_pages, writer):
    own_rows, col_width = outer_params.shape
    bits = islands.bit_length() - 1
    tiles = col_width // LANES
    page_count = own_rows * tiles
    capacity = 2 * page_count
    entries = islands * own_rows * col_width * tensor
    f32, bf16 = jnp.float32, jnp.bfloat16
    n_rs = len(cuts(page_count, SUBLANES, len(bit_orders(bits)) * ROUNDS))
    g_spans = cuts(page_count, 16, GATHER_CHUNKS)
    n_g = len(g_spans)
    n_lo = 1 << (bits // 2)
    n_hi = islands // n_lo
    dma = pltpu.SemaphoreType.DMA
    vmem = pl.BlockSpec(memory_space=pltpu.VMEM)
    smem = pl.BlockSpec(memory_space=pltpu.SMEM)

    def interleave(a):
        return a.reshape(-1, own_rows, tiles, LANES).swapaxes(1, 2).reshape(-1, page_count, LANES)

    def rows_of(a):
        return a.reshape(tiles, own_rows, LANES).swapaxes(0, 1).reshape(own_rows, col_width)

    x = pseudo_grad.reshape(-1, SUBLANES, tiles, LANES).swapaxes(1, 2)
    x = x.reshape(-1, tiles * SUBLANES, LANES)
    master, moment, packed = pl.pallas_call(
        functools.partial(kernel, bits, tensor, own_rows, entries),
        out_shape=(
            jax.ShapeDtypeStruct((page_count, LANES), f32),
            jax.ShapeDtypeStruct((page_count, LANES), f32),
            jax.ShapeDtypeStruct((capacity, LANES), bf16),
        ),
        in_specs=[pl.BlockSpec(memory_space=pl.ANY)] + [vmem] * 2 + [smem] * 2,
        out_specs=(vmem,) * 3,
        scratch_shapes=[pltpu.VMEM(x.shape, f32)]
        + [pltpu.VMEM((2,) * (bits - s) + (page_count, LANES), f32) for s in range(bits + 1)]
        + [pltpu.VMEM((n_hi, size, LANES), bf16) for _, size in g_spans]
        + [pltpu.VMEM((n_lo, size, LANES), bf16) for _, size in g_spans]
        + [pltpu.VMEM((n_lo, size, LANES), bf16) for _, size in g_spans]
        + [
            pltpu.VMEM((page_count, LANES), f32),
            pltpu.VMEM((page_count, LANES), f32),
            pltpu.VMEM((capacity + page_count, LANES), f32),
            pltpu.VMEM((islands * tensor, 8, LANES), f32),
            dma((n_rs, bits)),
            dma((n_rs, bits)),
            dma((islands * tensor,)),
            dma((islands * tensor,)),
            dma((n_g, 2, n_hi)),
            dma((n_g, 2, n_hi)),
            dma((n_g, n_lo)),
            dma((n_g, n_lo)),
            dma((n_rs,)),
        ],
        compiler_params=pltpu.CompilerParams(collective_id=0, has_side_effects=True),
    )(x, interleave(outer_params)[0], interleave(momentum)[0], save_pages, writer)
    master, moment, packed = pl.pallas_call(
        hand_on,
        out_shape=tuple(jax.ShapeDtypeStruct(a.shape, a.dtype) for a in (master, moment, packed)),
        in_specs=[vmem] * 3,
        out_specs=(vmem,) * 3,
    )(master, moment, packed)
    return rows_of(master), rows_of(moment), packed[None]


def solution(mesh):
    in_specs = (P("island", None, "tensor"), P("island", "tensor"), P("island", "tensor"), P(), P())
    out_specs = (P("island", "tensor"), P("island", "tensor"), P("island", None, "tensor"))
    step = functools.partial(body, mesh.shape["island"], mesh.shape["tensor"])
    return jax.shard_map(step, mesh=mesh, in_specs=in_specs, out_specs=out_specs, check_vma=False)
```
